32 devices in a mesh: section: 4 (over z), dp: 2 (over x), tensor: 4 (over y, core).
Axes of the slice: x: 2, y: 2, z: 4, core: 2. Of those that a mesh axis runs over, the one named last changes fastest.
Arguments:
- hidden: bfloat16 [64, 16384], P(('section', 'dp'), 'tensor'), may hold values from -100 to 100
- norm_gain: float32 [16384], replicated, may hold values from 0.5 to 1.5
- head_weight: bfloat16 [8192, 16384], P(('section', 'dp', 'tensor')), may hold values from -100 to 100
- token_ids: int32 [64], P(('section', 'dp')), may hold values from 0 to 8191
- resp_len: int32 [8, 2], P(('section', 'dp')), may hold values from 1 to 4, 6 in all within a row
- group_of: int32 [8, 2], P(('section', 'dp')), may hold values from 0 to 7
- loss_mask: int32 [64], P(('section', 'dp', 'tensor')), may hold values 0 or 1
- old_logp: float32 [64], P(('section', 'dp', 'tensor')), may hold values from -30 to 0
- ref_logp: float32 [64], P(('section', 'dp', 'tensor')), may hold values from -30 to 0
- advantage: float32 [64], P(('section', 'dp', 'tensor')), may hold values from -30 to 30
Outputs:
- token_logp: float32 [64], P(('section', 'dp', 'tensor'))
- group_loss: float32 [8], replicated
- group_count: float32 [8], replicated
The draws below stay inside these ranges and needn't reach their ends.
Inputs may be any that keep to these rules, and one draw needn't show every extreme that they name: `resp_len`: the response lengths of the 2 sequences of each shard sum to exactly 6.
All inputs are finite; a program needn't handle non-finite values. No bound on the sum of `loss_mask` on one device may be relied on, other than what follows from the above.
Results may differ from the reference program's by a relative error of at most 0.0003.
The reference program's roundings to bfloat16 on the way (of `normed`) count: a program that leaves them out, or rounds other values in their place, can miss the bound.
Values may be sent and summed in bfloat16 or wider, within the bound.
A program may use at most 128 MiB of HBM per device.

```python
import math
import jax
import jax.numpy as jnp
import numpy as np
from jax import lax

D = 16384
V_DEV = 256
VOCAB = 8192
WIN = 4
SEQ_SH = 2
GROUPS = 8
TOK_SH = 8
LIVE = 6
NSH = 8
TOK = 64


def head_row(key, row_id):
    return jax.random.normal(jax.random.fold_in(jax.random.fold_in(key, 7002), row_id), (D,), jnp.float32)


def draw_head_weight(key, part):
    entries = jax.vmap(lambda row_id: head_row(key, row_id))(jnp.arange(VOCAB))
    weights = entries / math.sqrt(D)
    return weights.astype(jnp.bfloat16)


def draw_hidden(key, part):
    values = jax.random.normal(jax.random.fold_in(key, 7003), (TOK, D), jnp.float32)
    values = jnp.clip(values, -6.0, 6.0)
    return values.astype(jnp.bfloat16)


def logp_draw(key, salt):
    spread = jax.random.uniform(jax.random.fold_in(key, salt), (TOK,), jnp.float32, -1.5, 1.5)
    return -math.log(VOCAB) - 0.5 + spread


def draw_old_logp(key, part):
    return logp_draw(key, 7004)


def draw_ref_logp(key, part):
    return logp_draw(key, 7005)


def draw_advantage(key, part):
    slope = jnp.arange(TOK).astype(jnp.float32) / max(TOK - 1, 1)
    values = jnp.clip(jax.random.normal(jax.random.fold_in(key, 7007), (TOK,), jnp.float32), -6.0, 6.0)
    return values * (1.0 + 2.0 * slope)


def touch_ends(drawn, rng, smallest, top_value):
    longest = drawn.shape.index(max(drawn.shape))
    spots = []
    for shift in (0, 1):
        where = [jax.random.randint(jax.random.fold_in(rng, axis), (), 0, length) for axis, length in enumerate(drawn.shape)]
        where[longest] = (where[longest] + shift) % drawn.shape[longest]
        spots.append(tuple(where))
    return drawn.at[spots[0]].set(smallest).at[spots[1]].set(top_value)


def rank_bounds(number_of, lean):
    loads = [(1 << 20) // math.isqrt(grade ** lean) + 1 for grade in range(1, number_of + 1)]
    deviation = 1 + sum(loads) // (1 << 30)
    return np.cumsum(np.array([max(1, weight // deviation) for weight in loads]))


def ranked_ids(key, dims, count, skew):
    listing = rank_bounds(count, skew)
    ticket = jax.random.randint(jax.random.fold_in(key, 1), dims, 0, int(listing[count - 1]))
    rank = jnp.searchsorted(jnp.asarray(listing, jnp.int32), ticket, side="right")
    return jax.random.permutation(jax.random.fold_in(key, 2), count)[rank].astype(jnp.int32)


def split_up(number_of, total, limit, skew):
    loads = [(1 << 20) // math.isqrt(grade ** skew) + 1 for grade in range(2, number_of + 1)]
    spare, counts = total - limit - (number_of - 1), [1] * (number_of - 1)
    while spare > 0:
        movable = [i for i in range(number_of - 1) if counts[i] < limit]
        mass, left = sum([loads[i] for i in movable]), spare
        for i in movable:
            addition = min(limit - counts[i], max(1, left * loads[i] // mass), spare)
            counts[i] = counts[i] + addition
            spare = spare - addition
    return np.array([limit] + counts)


def uneven(rng, number_of, total, limit, skew):
    if number_of == 2:
        one = jax.random.randint(rng, (), max(1, total - limit), min(limit, total - 1) + 1)
        return jnp.stack([one, total - one])
    sizes = jnp.asarray(split_up(number_of, total, limit, skew), jnp.int32)
    couples = (number_of - 1) // 2
    donor, receiver = sizes[1:1 + 2 * couples:2], sizes[2:2 + 2 * couples:2]
    room = jnp.minimum(donor - 1, limit - receiver)
    shifted = jax.random.randint(jax.random.fold_in(rng, 1), (couples,), 0, 1 << 20) % (room + 1)
    sizes = sizes.at[1:1 + 2 * couples:2].set(donor - shifted).at[2:2 + 2 * couples:2].set(receiver + shifted)
    return sizes[jax.random.permutation(jax.random.fold_in(rng, 2), number_of)]


def setup_inputs(seed: int = 0) -> dict:
    seeds = jax.random.split(jax.random.key(seed), 11)
    return {
        "hidden": draw_hidden(jax.random.fold_in(seeds[10], 71), 0),
        "norm_gain": jnp.clip(1.0 + 0.1 * jax.random.normal(seeds[1], (D,), jnp.float32), 0.5, 1.5),
        "head_weight": draw_head_weight(jax.random.fold_in(seeds[10], 71), 0),
        "token_ids": touch_ends(ranked_ids(seeds[3], (TOK,), VOCAB, 2), jax.random.fold_in(seeds[3], 3), 0, VOCAB - 1).astype(jnp.int32),
        "resp_len": jax.vmap(lambda own: uneven(own, SEQ_SH, LIVE, WIN, 0))(jax.random.split(seeds[4], NSH)).reshape((NSH, SEQ_SH)).astype(jnp.int32),
        "group_of": touch_ends(jax.random.randint(seeds[5], (NSH, SEQ_SH), 0, GROUPS), jax.random.fold_in(seeds[5], 1), 0, GROUPS - 1).astype(jnp.int32),
        "loss_mask": touch_ends((jax.random.randint(seeds[6], (TOK,), 0, 4) < 3).astype(jnp.int32), jax.random.fold_in(seeds[6], 1), 0, 1),
        "old_logp": draw_old_logp(jax.random.fold_in(seeds[10], 71), 0),
        "ref_logp": draw_ref_logp(jax.random.fold_in(seeds[10], 71), 0),
        "advantage": draw_advantage(jax.random.fold_in(seeds[10], 71), 0),
    }


epsilon = 1e-05
clip_range = 0.2
kl_weight = 0.1
log_clamp = 20.0

def normalize(hidden, norm_gain):
    values = hidden.astype(jnp.float32)
    mean_square = lax.optimization_barrier(jnp.mean(values * values, axis=1))
    return (values * lax.rsqrt(mean_square + epsilon)[:, None] * norm_gain[None, :]).astype(jnp.bfloat16)

def token_loss(logprob, old_logp, ref_logp, advantage, weight):
    ratios = jnp.exp(logprob - old_logp)
    clipped = jnp.clip(ratios, 1.0 - clip_range, 1.0 + clip_range)
    surrogate = jnp.minimum(ratios * advantage, clipped * advantage)
    log_gap = jnp.clip(ref_logp - logprob, -log_clamp, log_clamp)
    penalty = jnp.exp(log_gap) - log_gap - 1.0
    return (kl_weight * penalty - surrogate) * weight

def reference(hidden, norm_gain, head_weight, token_ids, resp_len, group_of, loss_mask, old_logp, ref_logp, advantage):
    normed = normalize(hidden, norm_gain)
    vocab_block = V_DEV * 32
    block_count = VOCAB // vocab_block
    blocks = head_weight.reshape(block_count, vocab_block, D)
    starts = (jnp.arange(block_count) * vocab_block).astype(jnp.int32)

    def absorb(carried, inputs):
        row_max, totals, chosen = carried
        weights, begin = inputs
        logits = jnp.dot(normed, weights.T, preferred_element_type=jnp.float32)
        column = begin + jnp.arange(vocab_block, dtype=jnp.int32)
        new_max = jnp.maximum(row_max, lax.optimization_barrier(jnp.max(logits, axis=1)))
        totals = totals * jnp.exp(row_max - new_max) + lax.optimization_barrier(jnp.sum(jnp.exp(logits - new_max[:, None]), axis=1))
        chosen = chosen + lax.optimization_barrier(jnp.sum(jnp.where(token_ids[:, None] == column[None, :], logits, 0.0), axis=1))
        return ((new_max, totals, chosen), None)
    initial = (jnp.full((TOK,), -jnp.inf, jnp.float32), jnp.zeros((TOK,), jnp.float32), jnp.zeros((TOK,), jnp.float32))
    (row_max, totals, chosen), unused = lax.scan(absorb, initial, (blocks, starts))
    logprob = chosen - (row_max + jnp.log(totals))
    position = jnp.arange(TOK, dtype=jnp.int32)
    local_row = position % TOK_SH
    seq_flat = position // TOK_SH * SEQ_SH + local_row // WIN
    within = local_row % WIN
    lengths = resp_len.reshape(-1)[seq_flat]
    is_live = within >= WIN - lengths
    token_logp = jnp.where(is_live, logprob, 0.0)
    weight = is_live.astype(jnp.float32) * loss_mask.astype(jnp.float32)
    losses = token_loss(logprob, old_logp, ref_logp, advantage, weight)
    groups = group_of.reshape(-1)[seq_flat]
    member = (groups[:, None] == jnp.arange(GROUPS, dtype=jnp.int32)[None, :]).astype(jnp.float32)
    group_loss = lax.optimization_barrier(jnp.sum(member * losses[:, None], axis=0))
    group_count = lax.optimization_barrier(jnp.sum(member * weight[:, None], axis=0))
    return (token_logp, group_loss, group_count)
```

```python
import functools

import jax
import jax.numpy as jnp
from jax import lax
from jax.experimental import pallas as pl
from jax.experimental.pallas import tpu as pltpu
from jax.sharding import PartitionSpec as P

GROUPS = 8
LANES = 128
MESH = pl.DeviceIdType.MESH
F32 = jnp.float32

epsilon = 1e-05
clip_range = 0.2
kl_weight = 0.1
log_clamp = 20.0


def token_loss(logprob, old_logp, ref_logp, advantage, weight):
    ratios = jnp.exp(logprob - old_logp)
    clipped = jnp.clip(ratios, 1.0 - clip_range, 1.0 + clip_range)
    surrogate = jnp.minimum(ratios * advantage, clipped * advantage)
    log_gap = jnp.clip(ref_logp - logprob, -log_clamp, log_clamp)
    penalty = jnp.exp(log_gap) - log_gap - 1.0
    return (kl_weight * penalty - surrogate) * weight


def pick(index, table):
    value = jnp.int32(table[0])
    for j in range(1, len(table)):
        value = jnp.where(index == j, jnp.int32(table[j]), value)
    return value


def kernel(
    sizes,
    hidden,
    gain,
    weight,
    token_ids,
    resp_len,
    group_of,
    loss_mask,
    old_logp,
    ref_logp,
    advantage,
    out_logp,
    out_loss,
    out_count,
    held,
    normed,
    head,
    gain_v,
    logits,
    meta_z,
    meta_x,
    meta_y,
    meta_c,
    stats,
    send_sem,
    recv_sem,
    meta_send,
    meta_recv,
    stat_send,
    stat_recv,
    local_sem,
):
    S, X, T = sizes
    C = 2
    Y = T // C
    N = S * X * T
    z, x, t = (lax.axis_index(a) for a in ("section", "dp", "tensor"))
    y, c = t // C, t % C
    rows, width = hidden.shape
    half = width // 2
    depth = width * T
    tokens = S * X * rows
    vocab = weight.shape[0]
    own_count = loss_mask.shape[0]
    me = (z * X + x) * T + t

    hidden_in = pltpu.make_async_copy(hidden, held.at[z, x, t], local_sem.at[0])
    hidden_in.start()
    gain_in = pltpu.make_async_copy(gain, gain_v, local_sem.at[1])
    gain_in.start()
    head_in = pltpu.make_async_copy(weight, head, local_sem.at[2])
    head_in.start()

    z_at = [z] + [lax.rem(z + d, S) for d in range(1, S)]
    x_at = [x] + [lax.rem(x + d, X) for d in range(1, X)]
    t_at = [t] + [lax.rem(t + d, T) for d in range(1, T)]
    y_at = [y] + [lax.rem(y + d, Y) for d in range(1, Y)]
    others = [
        (dz, dx, dt)
        for dz in range(S)
        for dx in range(X)
        for dt in range(T)
        if dz or dx or dt
    ]

    barrier = pltpu.get_barrier_semaphore()
    for dz, dx, dt in others:
        pl.semaphore_signal(
            barrier,
            inc=1,
            device_id={"section": z_at[dz], "dp": x_at[dx], "tensor": t_at[dt]},
            device_id_type=MESH,
        )

    lane = lax.broadcasted_iota(jnp.int32, (8, LANES * pl.cdiv(tokens, LANES)), 1)
    line = lax.broadcasted_iota(jnp.int32, lane.shape, 0)
    window = rows // resp_len.shape[1]
    own_start = (z * X + x) * rows + t * own_count
    meta = jnp.zeros(lane.shape, F32)
    for j in range(own_count):
        row = t * own_count + j
        within = row % window
        live = jnp.where(within >= window - resp_len[0, row // window], 1.0, 0.0)
        facts = (
            old_logp[j],
            ref_logp[j],
            advantage[j],
            live * loss_mask[j].astype(F32),
            group_of[0, row // window].astype(F32),
            token_ids[row].astype(F32),
            live,
        )
        value = jnp.zeros(lane.shape, F32)
        for i, fact in enumerate(facts):
            value = jnp.where(line == i, fact, value)
        meta = jnp.where(lane == own_start + j, value, meta)
    meta_z[z] = meta

    pl.semaphore_wait(barrier, N - 1)
    hidden_in.wait()

    sends = []

    def block(piece, bz, bx, by, bc):
        return held.at[bz, bx, by * C + bc, :, pl.ds(piece * half, half)]

    def describe(piece, bz, bx, by, bc, target):
        return pltpu.make_async_remote_copy(
            src_ref=block(piece, bz, bx, by, bc),
            dst_ref=block(piece, bz, bx, by, bc),
            send_sem=send_sem.at[len(sends)],
            recv_sem=recv_sem.at[piece, (bz * X + bx) * T + by * C + bc],
            device_id=target,
            device_id_type=MESH,
        )

    def send(piece, bz, bx, by, bc, target):
        copy = describe(piece, bz, bx, by, bc, target)
        copy.start()
        sends.append(copy)

    def arrived(piece, bz, bx, by, bc):
        pltpu.make_async_remote_copy(
            src_ref=block(piece, bz, bx, by, bc),
            dst_ref=block(piece, bz, bx, by, bc),
            send_sem=send_sem.at[0],
            recv_sem=recv_sem.at[piece, (bz * X + bx) * T + by * C + bc],
            device_id={"tensor": y * C + (1 - c)},
            device_id_type=MESH,
        ).wait_recv()

    to_x = [{"dp": x_at[d]} for d in range(1, X)]
    to_y = [{"tensor": y_at[d] * C + c} for d in range(1, Y)]
    to_c = [{"tensor": y * C + (1 - c)}]

    near = [sorted(range(S), key=lambda o, j=j: (abs(o - j), o)) for j in range(S)]
    z_near = [pick(z, [near[j][k] for j in range(S)]) for k in range(S)]

    meta_sends = []

    def meta_copy(buf, slot, order, target):
        return pltpu.make_async_remote_copy(
            src_ref=buf.at[slot],
            dst_ref=buf.at[slot],
            send_sem=meta_send.at[order],
            recv_sem=meta_recv.at[order],
            device_id=target,
            device_id_type=MESH,
        )

    def meta_phase(buf, mine, slots, targets, base):
        def put():
            for d, target in enumerate(targets):
                copy = pltpu.make_async_remote_copy(
                    src_ref=buf.at[mine],
                    dst_ref=buf.at[mine],
                    send_sem=meta_send.at[base + d],
                    recv_sem=meta_recv.at[base + d],
                    device_id=target,
                    device_id_type=MESH,
                )
                copy.start()
                meta_sends.append(copy)

        def take(following, slot):
            for d in range(len(targets)):
                meta_copy(buf, slots[-1 - d], base + d, targets[d]).wait_recv()
            following[slot] = jnp.sum(buf[...], axis=0)

        return put, take

    to_z = [{"section": z_at[d]} for d in range(1, S)]
    put_z, take_z = meta_phase(meta_z, z, z_at[1:], to_z, 0)
    put_x, take_x = meta_phase(meta_x, x, x_at[1:], to_x, S)
    put_y, take_y = meta_phase(meta_y, y, y_at[1:], to_y, S + X)
    put_c, take_c = meta_phase(meta_c, c, [1 - c], to_c, S + X + Y)
    errands = [
        put_z,
        lambda: take_z(meta_x, x),
        put_x,
        lambda: take_x(meta_y, y),
        put_y,
        lambda: take_y(meta_c, c),
        put_c,
    ]

    def from_z(bz, first):
        if not first:
            for piece in (0, 1):
                arrived(piece, bz, x, y, c)
        for target in to_x:
            send(0, bz, x, y, c, target)
        for target in to_y:
            send(1, bz, x, y, c, target)
        for target in to_x:
            send(1, bz, x, y, c, target)
        for target in to_y:
            send(0, bz, x, y, c, target)
        for piece in (0, 1):
            send(piece, bz, x, y, c, to_c[0])

    def from_plane(bz):
        for bx in x_at[1:]:
            arrived(0, bz, bx, y, c)
            for target in to_y + to_c:
                send(0, bz, bx, y, c, target)
        for by in y_at[1:]:
            arrived(1, bz, x, by, c)
            for target in to_x + to_c:
                send(1, bz, x, by, c, target)
        for bx in x_at[1:]:
            arrived(1, bz, bx, y, c)
            send(1, bz, bx, y, c, to_c[0])
        for by in y_at[1:]:
            arrived(0, bz, x, by, c)
            send(0, bz, x, by, c, to_c[0])

    def from_corner(bz):
        for bx in x_at[1:]:
            for by in y_at[1:]:
                for piece in (0, 1):
                    arrived(piece, bz, bx, by, c)
                    send(piece, bz, bx, by, c, to_c[0])

    step = min(width, 1024)

    def normalize(bz, first):
        if first:
            gain_in.wait()
        for bx in range(X):
            for by in range(Y):
                for piece in (0, 1):
                    arrived(piece, bz, bx, by, 1 - c)
        for pair in range(X // 2):
            def values(bt, col):
                return jnp.concatenate(
                    [
                        held[bz, 2 * pair + i, bt, :, pl.ds(col, step)].astype(F32)
                        for i in (0, 1)
                    ],
                    axis=0,
                )

            def squares(i, total):
                for bt in range(T):
                    v = values(bt, pl.multiple_of(i * step, step))
                    v = v * v
                    for k in range(step // LANES):
                        total = total + v[:, k * LANES : (k + 1) * LANES]
                return total

            total = lax.fori_loop(
                0, width // step, squares, jnp.zeros((2 * rows, LANES), F32)
            )
            mean_square = jnp.sum(total, axis=1, keepdims=True) / depth
            scale = lax.rsqrt(mean_square + epsilon)

            def write(i, carry):
                for bt in range(T):
                    col = pl.multiple_of(i * step, step)
                    at = pl.multiple_of(bt * width + i * step, step)
                    v = values(bt, col) * scale * gain_v[:, pl.ds(at, step)]
                    normed[bz * (X // 2) + pair, :, pl.ds(at, step)] = v.astype(jnp.bfloat16)
                return carry

            lax.fori_loop(0, width // step, write, 0)

    for bz in z_near[1:]:
        for piece in (0, 1):
            send(piece, z, x, y, c, {"section": bz})
    errands.pop(0)()
    for k in range(S + 3):
        if k < S:
            from_z(z_near[k], k == 0)
        if 0 <= k - 1 < S:
            from_plane(z_near[k - 1])
        if 0 <= k - 2 < S:
            from_corner(z_near[k - 2])
        if errands:
            errands.pop(0)()
        if 0 <= k - 3 < S:
            normalize(z_near[k - 3], k == 3)
    while errands:
        errands.pop(0)()

    head_in.wait()
    chunk = min(depth, 2048)
    logits[...] = jnp.zeros_like(logits)

    def multiply(i, carry):
        at = pl.multiple_of(i * chunk, chunk)
        part = normed[:, :, pl.ds(at, chunk)].reshape(tokens, chunk)
        logits[...] += lax.dot_general(
            head[:, pl.ds(at, chunk)],
            part,
            (((1,), (1,)), ((), ())),
            preferred_element_type=F32,
        )
        return carry

    lax.fori_loop(0, depth // chunk, multiply, 0)

    meta_copy(meta_c, 1 - c, S + X + Y, to_c[0]).wait_recv()
    meta = jnp.sum(meta_c[...], axis=0)
    facts = [meta[i : i + 1, :tokens] for i in range(7)]

    scores = logits[...]
    row_max = jnp.max(scores, axis=0, keepdims=True)
    totals = jnp.sum(jnp.exp(scores - row_max), axis=0, keepdims=True)
    entry = (lax.broadcasted_iota(jnp.int32, scores.shape, 0) + me * vocab).astype(F32)
    chosen = jnp.sum(jnp.where(entry == facts[5], scores, 0.0), axis=0, keepdims=True)
    padded = meta.shape[1]
    if padded > tokens:
        spare = jnp.zeros((1, padded - tokens), F32)
        row_max, totals, chosen = (
            jnp.concatenate([a, spare], axis=1) for a in (row_max, totals, chosen)
        )
    stats[me, :, :padded] = row_max
    stats[me, :, padded : 2 * padded] = totals
    stats[me, :, 2 * padded :] = chosen

    stat_sends = []
    for k, (dz, dx, dt) in enumerate(reversed(others)):
        copy = pltpu.make_async_remote_copy(
            src_ref=stats.at[me],
            dst_ref=stats.at[me],
            send_sem=stat_send.at[k],
            recv_sem=stat_recv.at[me],
            device_id={"section": z_at[dz], "dp": x_at[dx], "tensor": t_at[dt]},
            device_id_type=MESH,
        )
        copy.start()
        stat_sends.append(copy)
    for dz, dx, dt in others:
        source = (z_at[dz] * X + x_at[dx]) * T + t_at[dt]
        pltpu.make_async_remote_copy(
            src_ref=stats.at[source],
            dst_ref=stats.at[source],
            send_sem=stat_send.at[0],
            recv_sem=stat_recv.at[source],
            device_id=to_c[0],
            device_id_type=MESH,
        ).wait_recv()

    maxima = stats[:, :, :tokens]
    row_max = jnp.max(maxima, axis=0)
    totals = jnp.sum(
        stats[:, :, padded : padded + tokens] * jnp.exp(maxima - row_max[None]), axis=0
    )
    chosen = jnp.sum(stats[:, :, 2 * padded : 2 * padded + tokens], axis=0)
    logprob = chosen - (row_max + jnp.log(totals))
    old, ref, adv, counted, group, unused, live = facts
    losses = token_loss(logprob, old, ref, adv, counted)
    shown = jnp.where(live > 0.5, logprob, 0.0)

    def as_row(member, values, count):
        column = jnp.sum(jnp.where(member, values, 0.0), axis=1, keepdims=True)
        diagonal = lax.broadcasted_iota(jnp.int32, (8, LANES), 0) == lax.broadcasted_iota(
            jnp.int32, (8, LANES), 1
        )
        row = jnp.sum(jnp.where(diagonal, column, 0.0), axis=0, keepdims=True)
        return row[:, :count]

    line = lax.broadcasted_iota(jnp.int32, (8, tokens), 0)
    lane = lax.broadcasted_iota(jnp.int32, (8, tokens), 1)
    in_group = group == line.astype(F32)
    out_logp[...] = as_row(lane == own_start + line, shown, own_count)
    out_loss[...] = as_row(in_group, losses, GROUPS)
    out_count[...] = as_row(in_group, counted, GROUPS)

    for copy in sends + meta_sends + stat_sends:
        copy.wait_send()


def local(sizes, hidden, norm_gain, head_weight, *small):
    S, X, T = sizes
    N = S * X * T
    rows, width = hidden.shape
    depth = norm_gain.shape[0]
    vocab = head_weight.shape[0]
    tokens = S * X * rows
    own_count = small[3].shape[0]
    padded = LANES * pl.cdiv(tokens, LANES)
    Y = T // 2
    copies = 2 * (S - 1 + S * (X - 1) + S * X * (Y - 1) + S * X * Y)
    meta_count = S + X + Y + 2
    anywhere = pl.BlockSpec(memory_space=pl.ANY)
    smem = pl.BlockSpec(memory_space=pltpu.SMEM)
    vmem = pl.BlockSpec(memory_space=pltpu.VMEM)
    dma = pltpu.SemaphoreType.DMA
    logp, loss, count = pl.pallas_call(
        functools.partial(kernel, sizes),
        out_shape=(
            jax.ShapeDtypeStruct((1, own_count), F32),
            jax.ShapeDtypeStruct((1, GROUPS), F32),
            jax.ShapeDtypeStruct((1, GROUPS), F32),
        ),
        in_specs=[anywhere] * 3 + [smem] * 7,
        out_specs=(vmem, vmem, vmem),
        scratch_shapes=[
            pltpu.VMEM((S, X, T, rows, width), jnp.bfloat16),
            pltpu.VMEM((tokens // (2 * rows), 2 * rows, depth), jnp.bfloat16),
            pltpu.VMEM((vocab, depth), jnp.bfloat16),
            pltpu.VMEM((1, depth), F32),
            pltpu.VMEM((vocab, tokens), F32),
            pltpu.VMEM((S, 8, padded), F32),
            pltpu.VMEM((X, 8, padded), F32),
            pltpu.VMEM((Y, 8, padded), F32),
            pltpu.VMEM((2, 8, padded), F32),
            pltpu.VMEM((N, 1, 3 * padded), F32),
            dma((copies,)),
            dma((2, N)),
            dma((meta_count,)),
            dma((meta_count,)),
            dma((N - 1,)),
            dma((N,)),
            dma((3,)),
        ],
        compiler_params=pltpu.CompilerParams(
            collective_id=0, has_side_effects=True, vmem_limit_bytes=60 * 1024 * 1024
        ),
    )(hidden, norm_gain.reshape(1, depth), head_weight, *small)
    return logp.reshape(own_count), loss.reshape(GROUPS), count.reshape(GROUPS)


def solution(mesh):
    sizes = tuple(mesh.shape[a] for a in ("section", "dp", "tensor"))
    return jax.shard_map(
        functools.partial(local, sizes),
        mesh=mesh,
        in_specs=(
            P(("section", "dp"), "tensor"),
            P(),
            P(("section", "dp", "tensor"), None),
            P(("section", "dp")),
            P(("section", "dp"), None),
            P(("section", "dp"), None),
            P(("section", "dp", "tensor")),
            P(("section", "dp", "tensor")),
            P(("section", "dp", "tensor")),
            P(("section", "dp", "tensor")),
        ),
        out_specs=(P(("section", "dp", "tensor")), P(), P()),
        check_vma=False,
    )
```

```python
import functools

import jax
import jax.numpy as jnp
from jax import lax
from jax.experimental import pallas as pl
from jax.experimental.pallas import tpu as pltpu
from jax.sharding import PartitionSpec as P

GROUPS = 8
LANES = 128
MESH = pl.DeviceIdType.MESH
F32 = jnp.float32

epsilon = 1e-05
clip_range = 0.2
kl_weight = 0.1
log_clamp = 20.0


def token_loss(logprob, old_logp, ref_logp, advantage, weight):
    ratios = jnp.exp(logprob - old_logp)
    clipped = jnp.clip(ratios, 1.0 - clip_range, 1.0 + clip_range)
    surrogate = jnp.minimum(ratios * advantage, clipped * advantage)
    log_gap = jnp.clip(ref_logp - logprob, -log_clamp, log_clamp)
    penalty = jnp.exp(log_gap) - log_gap - 1.0
    return (kl_weight * penalty - surrogate) * weight


def pick(index, table):
    value = jnp.int32(table[0])
    for j in range(1, len(table)):
        value = jnp.where(index == j, jnp.int32(table[j]), value)
    return value


def kernel(
    sizes,
    hidden,
    gain,
    weight,
    token_ids,
    resp_len,
    group_of,
    loss_mask,
    old_logp,
    ref_logp,
    advantage,
    out,
    held,
    normed,
    head,
    gain_v,
    logits,
    meta_z,
    meta_x,
    meta_y,
    meta_c,
    stats,
    send_sem,
    recv_sem,
    meta_send,
    meta_recv,
    stat_send,
    stat_recv,
    local_sem,
):
    S, X, T = sizes
    C = 2
    Y = T // C
    N = S * X * T
    z, x, t = (lax.axis_index(a) for a in ("section", "dp", "tensor"))
    y, c = t // C, t % C
    rows, width = hidden.shape
    half = width // 2
    depth = width * T
    tokens = S * X * rows
    vocab = weight.shape[0]
    own_count = loss_mask.shape[0]
    me = (z * X + x) * T + t

    hidden_in = pltpu.make_async_copy(hidden, held.at[z, x, t], local_sem.at[0])
    hidden_in.start()
    gain_in = pltpu.make_async_copy(gain, gain_v, local_sem.at[1])
    gain_in.start()
    head_in = pltpu.make_async_copy(weight, head, local_sem.at[2])
    head_in.start()

    z_at = [z] + [lax.rem(z + d, S) for d in range(1, S)]
    x_at = [x] + [lax.rem(x + d, X) for d in range(1, X)]
    t_at = [t] + [lax.rem(t + d, T) for d in range(1, T)]
    y_at = [y] + [lax.rem(y + d, Y) for d in range(1, Y)]
    others = [
        (dz, dx, dt)
        for dz in range(S)
        for dx in range(X)
        for dt in range(T)
        if dz or dx or dt
    ]

    barrier = pltpu.get_barrier_semaphore()
    to_x = [{"dp": x_at[d]} for d in range(1, X)]
    to_y = [{"tensor": y_at[d] * C + c} for d in range(1, Y)]
    to_c = [{"tensor": y * C + (1 - c)}]
    to_z = [{"section": z_at[d]} for d in range(1, S)]
    for peer in to_z + to_x + to_y + to_c:
        pl.semaphore_signal(barrier, inc=1, device_id=peer, device_id_type=MESH)

    lane = lax.broadcasted_iota(jnp.int32, (8, LANES * pl.cdiv(tokens, LANES)), 1)
    line = lax.broadcasted_iota(jnp.int32, lane.shape, 0)
    window = rows // resp_len.shape[1]
    own_start = (z * X + x) * rows + t * own_count
    meta = jnp.zeros(lane.shape, F32)
    for j in range(own_count):
        row = t * own_count + j
        within = row % window
        live = jnp.where(within >= window - resp_len[0, row // window], 1.0, 0.0)
        facts = (
            old_logp[j],
            ref_logp[j],
            advantage[j],
            live * loss_mask[j].astype(F32),
            group_of[0, row // window].astype(F32),
            token_ids[row].astype(F32),
            live,
        )
        value = jnp.zeros(lane.shape, F32)
        for i, fact in enumerate(facts):
            value = jnp.where(line == i, fact, value)
        meta = jnp.where(lane == own_start + j, value, meta)
    meta_z[z] = meta

    pl.semaphore_wait(barrier, len(to_z + to_x + to_y + to_c))
    hidden_in.wait()

    sends = []

    def block(piece, bz, bx, by, bc):
        return held.at[bz, bx, by * C + bc, :, pl.ds(piece * half, half)]

    def describe(piece, bz, bx, by, bc, target):
        return pltpu.make_async_remote_copy(
            src_ref=block(piece, bz, bx, by, bc),
            dst_ref=block(piece, bz, bx, by, bc),
            send_sem=send_sem.at[len(sends)],
            recv_sem=recv_sem.at[piece, (bz * X + bx) * T + by * C + bc],
            device_id=target,
            device_id_type=MESH,
        )

    def send(piece, bz, bx, by, bc, target):
        copy = describe(piece, bz, bx, by, bc, target)
        copy.start()
        sends.append(copy)

    def arrived(piece, bz, bx, by, bc):
        pltpu.make_async_remote_copy(
            src_ref=block(piece, bz, bx, by, bc),
            dst_ref=block(piece, bz, bx, by, bc),
            send_sem=send_sem.at[0],
            recv_sem=recv_sem.at[piece, (bz * X + bx) * T + by * C + bc],
            device_id={"tensor": y * C + (1 - c)},
            device_id_type=MESH,
        ).wait_recv()

    near = [sorted(range(S), key=lambda o, j=j: (abs(o - j), o)) for j in range(S)]
    z_near = [pick(z, [near[j][k] for j in range(S)]) for k in range(S)]

    meta_sends = []

    def meta_copy(buf, slot, order, target):
        return pltpu.make_async_remote_copy(
            src_ref=buf.at[slot],
            dst_ref=buf.at[slot],
            send_sem=meta_send.at[order],
            recv_sem=meta_recv.at[order],
            device_id=target,
            device_id_type=MESH,
        )

    def meta_phase(buf, mine, slots, targets, base):
        def put():
            for d, target in enumerate(targets):
                copy = pltpu.make_async_remote_copy(
                    src_ref=buf.at[mine],
                    dst_ref=buf.at[mine],
                    send_sem=meta_send.at[base + d],
                    recv_sem=meta_recv.at[base + d],
                    device_id=target,
                    device_id_type=MESH,
                )
                copy.start()
                meta_sends.append(copy)

        def take(following, slot):
            for d in range(len(targets)):
                meta_copy(buf, slots[-1 - d], base + d, targets[d]).wait_recv()
            following[slot] = jnp.sum(buf[...], axis=0)

        return put, take

    put_z, take_z = meta_phase(meta_z, z, z_at[1:], to_z, 0)
    put_x, take_x = meta_phase(meta_x, x, x_at[1:], to_x, S)
    put_y, take_y = meta_phase(meta_y, y, y_at[1:], to_y, S + X)
    put_c, take_c = meta_phase(meta_c, c, [1 - c], to_c, S + X + Y)
    errands = [
        put_z,
        lambda: take_z(meta_x, x),
        put_x,
        lambda: take_x(meta_y, y),
        put_y,
        lambda: take_y(meta_c, c),
        put_c,
    ]

    def from_z(bz, first):
        if not first:
            for piece in (0, 1):
                arrived(piece, bz, x, y, c)
        for target in to_x:
            send(0, bz, x, y, c, target)
        for target in to_y:
            send(1, bz, x, y, c, target)
        for target in to_x:
            send(1, bz, x, y, c, target)
        for target in to_y:
            send(0, bz, x, y, c, target)
        for piece in (0, 1):
            send(piece, bz, x, y, c, to_c[0])

    def from_plane(bz):
        for bx in x_at[1:]:
            arrived(0, bz, bx, y, c)
            for target in to_y + to_c:
                send(0, bz, bx, y, c, target)
        for by in y_at[1:]:
            arrived(1, bz, x, by, c)
            for target in to_x + to_c:
                send(1, bz, x, by, c, target)
        for bx in x_at[1:]:
            arrived(1, bz, bx, y, c)
            send(1, bz, bx, y, c, to_c[0])
        for by in y_at[1:]:
            arrived(0, bz, x, by, c)
            send(0, bz, x, by, c, to_c[0])

    def from_corner(bz):
        for bx in x_at[1:]:
            for by in y_at[1:]:
                for piece in (0, 1):
                    arrived(piece, bz, bx, by, c)
                    send(piece, bz, bx, by, c, to_c[0])

    step = min(width, 1024)

    def normalize(bz, first):
        if first:
            gain_in.wait()
        for bx in range(X):
            for by in range(Y):
                for piece in (0, 1):
                    arrived(piece, bz, bx, by, 1 - c)
        for pair in range(X // 2):
            def values(bt, col):
                return jnp.concatenate(
                    [
                        held[bz, 2 * pair + i, bt, :, pl.ds(col, step)].astype(F32)
                        for i in (0, 1)
                    ],
                    axis=0,
                )

            def squares(i, total):
                for bt in range(T):
                    v = values(bt, pl.multiple_of(i * step, step))
                    v = v * v
                    for k in range(step // LANES):
                        total = total + v[:, k * LANES : (k + 1) * LANES]
                return total

            total = lax.fori_loop(
                0, width // step, squares, jnp.zeros((2 * rows, LANES), F32)
            )
            mean_square = jnp.sum(total, axis=1, keepdims=True) / depth
            scale = lax.rsqrt(mean_square + epsilon)

            def write(i, carry):
                for bt in range(T):
                    col = pl.multiple_of(i * step, step)
                    at = pl.multiple_of(bt * width + i * step, step)
                    v = values(bt, col) * scale * gain_v[:, pl.ds(at, step)]
                    normed[bz * (X // 2) + pair, :, pl.ds(at, step)] = v.astype(jnp.bfloat16)
                return carry

            lax.fori_loop(0, width // step, write, 0)

    for bz in z_near[1:]:
        for piece in (0, 1):
            send(piece, z, x, y, c, {"section": bz})
    errands.pop(0)()
    for k in range(S + 3):
        if k < S:
            from_z(z_near[k], k == 0)
        if 0 <= k - 1 < S:
            from_plane(z_near[k - 1])
        if 0 <= k - 2 < S:
            from_corner(z_near[k - 2])
        if errands:
            errands.pop(0)()
        if 0 <= k - 3 < S:
            normalize(z_near[k - 3], k == 3)
    while errands:
        errands.pop(0)()

    head_in.wait()
    chunk = min(depth, 2048)
    logits[...] = jnp.zeros_like(logits)

    def multiply(i, carry):
        at = pl.multiple_of(i * chunk, chunk)
        part = normed[:, :, pl.ds(at, chunk)].reshape(tokens, chunk)
        logits[...] += lax.dot_general(
            head[:, pl.ds(at, chunk)],
            part,
            (((1,), (1,)), ((), ())),
            preferred_element_type=F32,
        )
        return carry

    lax.fori_loop(0, depth // chunk, multiply, 0)

    meta_copy(meta_c, 1 - c, S + X + Y, to_c[0]).wait_recv()
    meta = jnp.sum(meta_c[...], axis=0)
    facts = [meta[i : i + 1, :tokens] for i in range(7)]

    scores = logits[...]
    row_max = jnp.max(scores, axis=0, keepdims=True)
    totals = jnp.sum(jnp.exp(scores - row_max), axis=0, keepdims=True)
    entry = (lax.broadcasted_iota(jnp.int32, scores.shape, 0) + me * vocab).astype(F32)
    chosen = jnp.sum(jnp.where(entry == facts[5], scores, 0.0), axis=0, keepdims=True)
    padded = meta.shape[1]
    if padded > tokens:
        spare = jnp.zeros((1, padded - tokens), F32)
        row_max, totals, chosen = (
            jnp.concatenate([a, spare], axis=1) for a in (row_max, totals, chosen)
        )
    stats[me, :, :padded] = row_max
    stats[me, :, padded : 2 * padded] = totals
    stats[me, :, 2 * padded :] = chosen

    stat_sends = []
    for k, (dz, dx, dt) in enumerate(reversed(others)):
        copy = pltpu.make_async_remote_copy(
            src_ref=stats.at[me],
            dst_ref=stats.at[me],
            send_sem=stat_send.at[k],
            recv_sem=stat_recv.at[me],
            device_id={"section": z_at[dz], "dp": x_at[dx], "tensor": t_at[dt]},
            device_id_type=MESH,
        )
        copy.start()
        stat_sends.append(copy)
    for dz, dx, dt in others:
        source = (z_at[dz] * X + x_at[dx]) * T + t_at[dt]
        pltpu.make_async_remote_copy(
            src_ref=stats.at[source],
            dst_ref=stats.at[source],
            send_sem=stat_send.at[0],
            recv_sem=stat_recv.at[source],
            device_id=to_c[0],
            device_id_type=MESH,
        ).wait_recv()

    maxima = stats[:, :, :tokens]
    row_max = jnp.max(maxima, axis=0)
    totals = jnp.sum(
        stats[:, :, padded : padded + tokens] * jnp.exp(maxima - row_max[None]), axis=0
    )
    chosen = jnp.sum(stats[:, :, 2 * padded : 2 * padded + tokens], axis=0)
    logprob = chosen - (row_max + jnp.log(totals))
    old, ref, adv, counted, group, unused, live = facts
    losses = token_loss(logprob, old, ref, adv, counted)
    shown = jnp.where(live > 0.5, logprob, 0.0)

    def as_row(member, values):
        column = jnp.sum(jnp.where(member, values, 0.0), axis=1, keepdims=True)
        diagonal = lax.broadcasted_iota(jnp.int32, (8, LANES), 0) == lax.broadcasted_iota(
            jnp.int32, (8, LANES), 1
        )
        return jnp.sum(jnp.where(diagonal, column, 0.0), axis=0, keepdims=True)

    line = lax.broadcasted_iota(jnp.int32, (8, tokens), 0)
    lane = lax.broadcasted_iota(jnp.int32, (8, tokens), 1)
    in_group = group == line.astype(F32)
    out[...] = jnp.zeros_like(out)
    out[0:1, :] = as_row(lane == own_start + line, shown)
    out[1:2, :] = as_row(in_group, losses)
    out[2:3, :] = as_row(in_group, counted)

    for copy in sends + meta_sends + stat_sends:
        copy.wait_send()


def spread(packed, out_logp, out_loss, out_count):
    out_logp[...] = packed[0:1, : out_logp.shape[1]]
    out_loss[...] = packed[1:2, : out_loss.shape[1]]
    out_count[...] = packed[2:3, : out_count.shape[1]]


def local(sizes, hidden, norm_gain, head_weight, *small):
    S, X, T = sizes
    N = S * X * T
    rows, width = hidden.shape
    depth = norm_gain.shape[0]
    vocab = head_weight.shape[0]
    tokens = S * X * rows
    own_count = small[3].shape[0]
    padded = LANES * pl.cdiv(tokens, LANES)
    Y = T // 2
    copies = 2 * (S - 1 + S * (X - 1) + S * X * (Y - 1) + S * X * Y)
    meta_count = S + X + Y + 2
    anywhere = pl.BlockSpec(memory_space=pl.ANY)
    smem = pl.BlockSpec(memory_space=pltpu.SMEM)
    vmem = pl.BlockSpec(memory_space=pltpu.VMEM)
    dma = pltpu.SemaphoreType.DMA
    packed = pl.pallas_call(
        functools.partial(kernel, sizes),
        out_shape=jax.ShapeDtypeStruct((8, LANES), F32),
        in_specs=[anywhere] * 3 + [smem] * 7,
        out_specs=vmem,
        scratch_shapes=[
            pltpu.VMEM((S, X, T, rows, width), jnp.bfloat16),
            pltpu.VMEM((tokens // (2 * rows), 2 * rows, depth), jnp.bfloat16),
            pltpu.VMEM((vocab, depth), jnp.bfloat16),
            pltpu.VMEM((1, depth), F32),
            pltpu.VMEM((vocab, tokens), F32),
            pltpu.VMEM((S, 8, padded), F32),
            pltpu.VMEM((X, 8, padded), F32),
            pltpu.VMEM((Y, 8, padded), F32),
            pltpu.VMEM((2, 8, padded), F32),
            pltpu.VMEM((N, 1, 3 * padded), F32),
            dma((copies,)),
            dma((2, N)),
            dma((meta_count,)),
            dma((meta_count,)),
            dma((N - 1,)),
            dma((N,)),
            dma((3,)),
        ],
        compiler_params=pltpu.CompilerParams(
            collective_id=0, has_side_effects=True, vmem_limit_bytes=60 * 1024 * 1024
        ),
    )(hidden, norm_gain.reshape(1, depth), head_weight, *small)
    logp, loss, count = pl.pallas_call(
        spread,
        out_shape=(
            jax.ShapeDtypeStruct((1, own_count), F32),
            jax.ShapeDtypeStruct((1, GROUPS), F32),
            jax.ShapeDtypeStruct((1, GROUPS), F32),
        ),
        in_specs=[vmem],
        out_specs=(vmem, vmem, vmem),
    )(packed)
    return logp.reshape(own_count), loss.reshape(GROUPS), count.reshape(GROUPS)


def solution(mesh):
    sizes = tuple(mesh.shape[a] for a in ("section", "dp", "tensor"))
    return jax.shard_map(
        functools.partial(local, sizes),
        mesh=mesh,
        in_specs=(
            P(("section", "dp"), "tensor"),
            P(),
            P(("section", "dp", "tensor"), None),
            P(("section", "dp")),
            P(("section", "dp"), None),
            P(("section", "dp"), None),
            P(("section", "dp", "tensor")),
            P(("section", "dp", "tensor")),
            P(("section", "dp", "tensor")),
            P(("section", "dp", "tensor")),
        ),
        out_specs=(P(("section", "dp", "tensor")), P(), P()),
        check_vma=False,
    )
```

```python
import functools

import jax
import jax.numpy as jnp
from jax import lax
from jax.experimental import pallas as pl
from jax.experimental.pallas import tpu as pltpu
from jax.sharding import PartitionSpec as P

GROUPS = 8
LANES = 128
MESH = pl.DeviceIdType.MESH
F32 = jnp.float32

epsilon = 1e-05
clip_range = 0.2
kl_weight = 0.1
log_clamp = 20.0


def token_loss(logprob, old_logp, ref_logp, advantage, weight):
    ratios = jnp.exp(logprob - old_logp)
    clipped = jnp.clip(ratios, 1.0 - clip_range, 1.0 + clip_range)
    surrogate = jnp.minimum(ratios * advantage, clipped * advantage)
    log_gap = jnp.clip(ref_logp - logprob, -log_clamp, log_clamp)
    penalty = jnp.exp(log_gap) - log_gap - 1.0
    return (kl_weight * penalty - surrogate) * weight


def pick(index, table):
    value = jnp.int32(table[0])
    for j in range(1, len(table)):
        value = jnp.where(index == j, jnp.int32(table[j]), value)
    return value


def kernel(
    sizes,
    hidden,
    gain,
    weight,
    token_ids,
    resp_len,
    group_of,
    loss_mask,
    old_logp,
    ref_logp,
    advantage,
    out,
    held,
    normed,
    head,
    gain_v,
    logits,
    meta_z,
    meta_x,
    meta_y,
    meta_c,
    stats,
    send_sem,
    recv_sem,
    meta_send,
    meta_recv,
    stat_send,
    stat_recv,
    local_sem,
    *small_s,
):
    S, X, T = sizes
    C = 2
    Y = T // C
    N = S * X * T
    z, x, t = (lax.axis_index(a) for a in ("section", "dp", "tensor"))
    y, c = t // C, t % C
    rows, width = hidden.shape
    half = width // 2
    depth = width * T
    tokens = S * X * rows
    vocab = weight.shape[0]
    own_count = loss_mask.shape[0]
    me = (z * X + x) * T + t

    hidden_in = pltpu.make_async_copy(hidden, held.at[z, x, t], local_sem.at[0])
    hidden_in.start()
    small = (token_ids, resp_len, group_of, loss_mask, old_logp, ref_logp, advantage)
    small_in = [
        pltpu.make_async_copy(a, b, local_sem.at[3 + i])
        for i, (a, b) in enumerate(zip(small, small_s))
    ]
    for copy in small_in:
        copy.start()
    token_ids, resp_len, group_of, loss_mask, old_logp, ref_logp, advantage = small_s
    gain_in = pltpu.make_async_copy(gain, gain_v, local_sem.at[1])
    gain_in.start()
    head_in = pltpu.make_async_copy(weight, head, local_sem.at[2])
    head_in.start()

    z_at = [z] + [lax.rem(z + d, S) for d in range(1, S)]
    x_at = [x] + [lax.rem(x + d, X) for d in range(1, X)]
    t_at = [t] + [lax.rem(t + d, T) for d in range(1, T)]
    y_at = [y] + [lax.rem(y + d, Y) for d in range(1, Y)]
    others = [
        (dz, dx, dt)
        for dz in range(S)
        for dx in range(X)
        for dt in range(T)
        if dz or dx or dt
    ]

    barrier = pltpu.get_barrier_semaphore()
    to_x = [{"dp": x_at[d]} for d in range(1, X)]
    to_y = [{"tensor": y_at[d] * C + c} for d in range(1, Y)]
    to_c = [{"tensor": y * C + (1 - c)}]
    to_z = [{"section": z_at[d]} for d in range(1, S)]
    for peer in to_z + to_x + to_y + to_c:
        pl.semaphore_signal(barrier, inc=1, device_id=peer, device_id_type=MESH)

    pl.semaphore_wait(barrier, len(to_z + to_x + to_y + to_c))
    hidden_in.wait()

    sends = []

    def block(piece, bz, bx, by, bc):
        return held.at[bz, bx, by * C + bc, :, pl.ds(piece * half, half)]

    def describe(piece, bz, bx, by, bc, target):
        return pltpu.make_async_remote_copy(
            src_ref=block(piece, bz, bx, by, bc),
            dst_ref=block(piece, bz, bx, by, bc),
            send_sem=send_sem.at[len(sends)],
            recv_sem=recv_sem.at[piece, (bz * X + bx) * T + by * C + bc],
            device_id=target,
            device_id_type=MESH,
        )

    def send(piece, bz, bx, by, bc, target):
        copy = describe(piece, bz, bx, by, bc, target)
        copy.start()
        sends.append(copy)

    def arrived(piece, bz, bx, by, bc):
        pltpu.make_async_remote_copy(
            src_ref=block(piece, bz, bx, by, bc),
            dst_ref=block(piece, bz, bx, by, bc),
            send_sem=send_sem.at[0],
            recv_sem=recv_sem.at[piece, (bz * X + bx) * T + by * C + bc],
            device_id={"tensor": y * C + (1 - c)},
            device_id_type=MESH,
        ).wait_recv()

    near = [sorted(range(S), key=lambda o, j=j: (abs(o - j), o)) for j in range(S)]
    z_near = [pick(z, [near[j][k] for j in range(S)]) for k in range(S)]

    meta_sends = []

    def meta_copy(buf, slot, order, target):
        return pltpu.make_async_remote_copy(
            src_ref=buf.at[slot],
            dst_ref=buf.at[slot],
            send_sem=meta_send.at[order],
            recv_sem=meta_recv.at[order],
            device_id=target,
            device_id_type=MESH,
        )

    def meta_phase(buf, mine, slots, targets, base):
        def put():
            for d, target in enumerate(targets):
                copy = pltpu.make_async_remote_copy(
                    src_ref=buf.at[mine],
                    dst_ref=buf.at[mine],
                    send_sem=meta_send.at[base + d],
                    recv_sem=meta_recv.at[base + d],
                    device_id=target,
                    device_id_type=MESH,
                )
                copy.start()
                meta_sends.append(copy)

        def take(following, slot):
            for d in range(len(targets)):
                meta_copy(buf, slots[-1 - d], base + d, targets[d]).wait_recv()
            following[slot] = jnp.sum(buf[...], axis=0)

        return put, take

    put_z, take_z = meta_phase(meta_z, z, z_at[1:], to_z, 0)
    put_x, take_x = meta_phase(meta_x, x, x_at[1:], to_x, S)
    put_y, take_y = meta_phase(meta_y, y, y_at[1:], to_y, S + X)
    put_c, take_c = meta_phase(meta_c, c, [1 - c], to_c, S + X + Y)
    errands = [
        put_z,
        lambda: take_z(meta_x, x),
        put_x,
        lambda: take_x(meta_y, y),
        put_y,
        lambda: take_y(meta_c, c),
        put_c,
    ]

    def from_z(bz, first):
        if not first:
            for piece in (0, 1):
                arrived(piece, bz, x, y, c)
        for target in to_x:
            send(0, bz, x, y, c, target)
        for target in to_y:
            send(1, bz, x, y, c, target)
        for target in to_x:
            send(1, bz, x, y, c, target)
        for target in to_y:
            send(0, bz, x, y, c, target)
        for piece in (0, 1):
            send(piece, bz, x, y, c, to_c[0])

    def from_plane(bz):
        for bx in x_at[1:]:
            arrived(0, bz, bx, y, c)
            for target in to_y + to_c:
                send(0, bz, bx, y, c, target)
        for by in y_at[1:]:
            arrived(1, bz, x, by, c)
            for target in to_x + to_c:
                send(1, bz, x, by, c, target)
        for bx in x_at[1:]:
            arrived(1, bz, bx, y, c)
            send(1, bz, bx, y, c, to_c[0])
        for by in y_at[1:]:
            arrived(0, bz, x, by, c)
            send(0, bz, x, by, c, to_c[0])

    def from_corner(bz):
        for bx in x_at[1:]:
            for by in y_at[1:]:
                for piece in (0, 1):
                    arrived(piece, bz, bx, by, c)
                    send(piece, bz, bx, by, c, to_c[0])

    step = min(width, 1024)

    def normalize(bz, first):
        if first:
            gain_in.wait()
        for bx in range(X):
            for by in range(Y):
                for piece in (0, 1):
                    arrived(piece, bz, bx, by, 1 - c)
        for pair in range(X // 2):
            def values(bt, col):
                return jnp.concatenate(
                    [
                        held[bz, 2 * pair + i, bt, :, pl.ds(col, step)].astype(F32)
                        for i in (0, 1)
                    ],
                    axis=0,
                )

            def squares(i, total):
                for bt in range(T):
                    v = values(bt, pl.multiple_of(i * step, step))
                    v = v * v
                    for k in range(step // LANES):
                        total = total + v[:, k * LANES : (k + 1) * LANES]
                return total

            total = lax.fori_loop(
                0, width // step, squares, jnp.zeros((2 * rows, LANES), F32)
            )
            mean_square = jnp.sum(total, axis=1, keepdims=True) / depth
            scale = lax.rsqrt(mean_square + epsilon)

            def write(i, carry):
                for bt in range(T):
                    col = pl.multiple_of(i * step, step)
                    at = pl.multiple_of(bt * width + i * step, step)
                    v = values(bt, col) * scale * gain_v[:, pl.ds(at, step)]
                    normed[bz * (X // 2) + pair, :, pl.ds(at, step)] = v.astype(jnp.bfloat16)
                return carry

            lax.fori_loop(0, width // step, write, 0)

    for bz in z_near[1:]:
        for piece in (0, 1):
            send(piece, z, x, y, c, {"section": bz})
    for k in range(S + 3):
        if k < S:
            from_z(z_near[k], k == 0)
        if k == 0:
            lane = lax.broadcasted_iota(jnp.int32, (8, LANES * pl.cdiv(tokens, LANES)), 1)
            line = lax.broadcasted_iota(jnp.int32, lane.shape, 0)
            window = rows // resp_len.shape[1]
            own_start = (z * X + x) * rows + t * own_count
            for copy in small_in:
                copy.wait()
            meta = jnp.zeros(lane.shape, F32)
            for j in range(own_count):
                row = t * own_count + j
                within = row % window
                live = jnp.where(within >= window - resp_len[0, row // window], 1.0, 0.0)
                facts = (
                    old_logp[j],
                    ref_logp[j],
                    advantage[j],
                    live * loss_mask[j].astype(F32),
                    group_of[0, row // window].astype(F32),
                    token_ids[row].astype(F32),
                    live,
                )
                value = jnp.zeros(lane.shape, F32)
                for i, fact in enumerate(facts):
                    value = jnp.where(line == i, fact, value)
                meta = jnp.where(lane == own_start + j, value, meta)
            meta_z[z] = meta
        if 0 <= k - 1 < S:
            from_plane(z_near[k - 1])
        if 0 <= k - 2 < S:
            from_corner(z_near[k - 2])
        if errands:
            errands.pop(0)()
        if 0 <= k - 3 < S:
            normalize(z_near[k - 3], k == 3)
    while errands:
        errands.pop(0)()

    head_in.wait()
    chunk = min(depth, 8192)
    logits[...] = jnp.zeros_like(logits)

    def multiply(i, carry):
        at = pl.multiple_of(i * chunk, chunk)
        part = normed[:, :, pl.ds(at, chunk)].reshape(tokens, chunk)
        logits[...] += lax.dot_general(
            head[:, pl.ds(at, chunk)],
            part,
            (((1,), (1,)), ((), ())),
            preferred_element_type=F32,
        )
        return carry

    lax.fori_loop(0, depth // chunk, multiply, 0)

    meta_copy(meta_c, 1 - c, S + X + Y, to_c[0]).wait_recv()
    meta = jnp.sum(meta_c[...], axis=0)
    facts = [meta[i : i + 1, :tokens] for i in range(7)]

    scores = logits[...]
    row_max = jnp.max(scores, axis=0, keepdims=True)
    totals = jnp.sum(jnp.exp(scores - row_max), axis=0, keepdims=True)
    entry = (lax.broadcasted_iota(jnp.int32, scores.shape, 0) + me * vocab).astype(F32)
    chosen = jnp.sum(jnp.where(entry == facts[5], scores, 0.0), axis=0, keepdims=True)
    padded = meta.shape[1]
    if padded > tokens:
        spare = jnp.zeros((1, padded - tokens), F32)
        row_max, totals, chosen = (
            jnp.concatenate([a, spare], axis=1) for a in (row_max, totals, chosen)
        )
    stats[me, :, :padded] = row_max
    stats[me, :, padded : 2 * padded] = totals
    stats[me, :, 2 * padded :] = chosen

    stat_sends = []
    for k, (dz, dx, dt) in enumerate(reversed(others)):
        copy = pltpu.make_async_remote_copy(
            src_ref=stats.at[me],
            dst_ref=stats.at[me],
            send_sem=stat_send.at[k],
            recv_sem=stat_recv.at[me],
            device_id={"section": z_at[dz], "dp": x_at[dx], "tensor": t_at[dt]},
            device_id_type=MESH,
        )
        copy.start()
        stat_sends.append(copy)
    for dz, dx, dt in others:
        source = (z_at[dz] * X + x_at[dx]) * T + t_at[dt]
        pltpu.make_async_remote_copy(
            src_ref=stats.at[source],
            dst_ref=stats.at[source],
            send_sem=stat_send.at[0],
            recv_sem=stat_recv.at[source],
            device_id=to_c[0],
            device_id_type=MESH,
        ).wait_recv()

    maxima = stats[:, :, :tokens]
    row_max = jnp.max(maxima, axis=0)
    totals = jnp.sum(
        stats[:, :, padded : padded + tokens] * jnp.exp(maxima - row_max[None]), axis=0
    )
    chosen = jnp.sum(stats[:, :, 2 * padded : 2 * padded + tokens], axis=0)
    logprob = chosen - (row_max + jnp.log(totals))
    old, ref, adv, counted, group, unused, live = facts
    losses = token_loss(logprob, old, ref, adv, counted)
    shown = jnp.where(live > 0.5, logprob, 0.0)

    def as_row(member, values):
        column = jnp.sum(jnp.where(member, values, 0.0), axis=1, keepdims=True)
        diagonal = lax.broadcasted_iota(jnp.int32, (8, LANES), 0) == lax.broadcasted_iota(
            jnp.int32, (8, LANES), 1
        )
        return jnp.sum(jnp.where(diagonal, column, 0.0), axis=0, keepdims=True)

    line = lax.broadcasted_iota(jnp.int32, (8, tokens), 0)
    lane = lax.broadcasted_iota(jnp.int32, (8, tokens), 1)
    in_group = group == line.astype(F32)
    out[...] = jnp.zeros_like(out)
    out[0:1, :] = as_row(lane == own_start + line, shown)
    out[1:2, :] = as_row(in_group, losses)
    out[2:3, :] = as_row(in_group, counted)

    for copy in sends + meta_sends + stat_sends:
        copy.wait_send()


def spread(packed, out_logp, out_loss, out_count):
    out_logp[...] = packed[0:1, : out_logp.shape[1]]
    out_loss[...] = packed[1:2, : out_loss.shape[1]]
    out_count[...] = packed[2:3, : out_count.shape[1]]


def local(sizes, hidden, norm_gain, head_weight, *small):
    S, X, T = sizes
    N = S * X * T
    rows, width = hidden.shape
    depth = norm_gain.shape[0]
    vocab = head_weight.shape[0]
    tokens = S * X * rows
    own_count = small[3].shape[0]
    padded = LANES * pl.cdiv(tokens, LANES)
    Y = T // 2
    copies = 2 * (S - 1 + S * (X - 1) + S * X * (Y - 1) + S * X * Y)
    meta_count = S + X + Y + 2
    anywhere = pl.BlockSpec(memory_space=pl.ANY)
    vmem = pl.BlockSpec(memory_space=pltpu.VMEM)
    dma = pltpu.SemaphoreType.DMA
    packed = pl.pallas_call(
        functools.partial(kernel, sizes),
        out_shape=jax.ShapeDtypeStruct((8, LANES), F32),
        in_specs=[anywhere] * 10,
        out_specs=vmem,
        scratch_shapes=[
            pltpu.VMEM((S, X, T, rows, width), jnp.bfloat16),
            pltpu.VMEM((tokens // (2 * rows), 2 * rows, depth), jnp.bfloat16),
            pltpu.VMEM((vocab, depth), jnp.bfloat16),
            pltpu.VMEM((1, depth), F32),
            pltpu.VMEM((vocab, tokens), F32),
            pltpu.VMEM((S, 8, padded), F32),
            pltpu.VMEM((X, 8, padded), F32),
            pltpu.VMEM((Y, 8, padded), F32),
            pltpu.VMEM((2, 8, padded), F32),
            pltpu.VMEM((N, 1, 3 * padded), F32),
            dma((copies,)),
            dma((2, N)),
            dma((meta_count,)),
            dma((meta_count,)),
            dma((N - 1,)),
            dma((N,)),
            dma((3 + len(small),)),
        ]
        + [pltpu.SMEM(a.shape, a.dtype) for a in small],
        compiler_params=pltpu.CompilerParams(
            collective_id=0, has_side_effects=True, vmem_limit_bytes=60 * 1024 * 1024
        ),
    )(hidden, norm_gain.reshape(1, depth), head_weight, *small)
    logp, loss, count = pl.pallas_call(
        spread,
        out_shape=(
            jax.ShapeDtypeStruct((1, own_count), F32),
            jax.ShapeDtypeStruct((1, GROUPS), F32),
            jax.ShapeDtypeStruct((1, GROUPS), F32),
        ),
        in_specs=[vmem],
        out_specs=(vmem, vmem, vmem),
    )(packed)
    return logp.reshape(own_count), loss.reshape(GROUPS), count.reshape(GROUPS)


def solution(mesh):
    sizes = tuple(mesh.shape[a] for a in ("section", "dp", "tensor"))
    return jax.shard_map(
        functools.partial(local, sizes),
        mesh=mesh,
        in_specs=(
            P(("section", "dp"), "tensor"),
            P(),
            P(("section", "dp", "tensor"), None),
            P(("section", "dp")),
            P(("section", "dp"), None),
            P(("section", "dp"), None),
            P(("section", "dp", "tensor")),
            P(("section", "dp", "tensor")),
            P(("section", "dp", "tensor")),
            P(("section", "dp", "tensor")),
        ),
        out_specs=(P(("section", "dp", "tensor")), P(), P()),
        check_vma=False,
    )
```
